32 devices in a mesh: bank: 4 (over y, core), zero: 8 (over z, x).
Axes of the slice: x: 2, y: 2, z: 4, core: 2. Of those that a mesh axis runs over, the one named last changes fastest.
Arguments:
- train_gate: float32 [128, 2048, 768], P('bank', 'zero'), may hold values from -0.1875 to 0.1875
- other_gate: bfloat16 [128, 2048, 768], P('bank', 'zero'), may hold values from -0.0625 to 0.0625
- train_up: float32 [128, 2048, 768], P('bank', 'zero'), may hold values from -0.1875 to 0.1875
- other_up: bfloat16 [128, 2048, 768], P('bank', 'zero'), may hold values from -0.0625 to 0.0625
- router_weight: float32 [2048, 128], P('zero', 'bank'), may hold values from -0.125 to 0.125
- router_gain: float32 [2048], P('zero'), may hold values from 0.25 to 1.75
Outputs:
- ready_gate: bfloat16 [128, 2048, 768], P(('bank', 'zero'))
- ready_up: bfloat16 [128, 2048, 768], P(('bank', 'zero'))
- scale_gate: float32 [128, 768], P(('bank', 'zero'))
- scale_up: float32 [128, 768], P(('bank', 'zero'))
- serve_router: bfloat16 [2048, 128], replicated
The draws below stay inside these ranges and needn't reach their ends.
All inputs are finite; a program needn't handle non-finite values.
Results may differ from the reference program's by a relative error of at most 0.0075.
Values may be sent and summed in bfloat16 or wider, within the bound.
A program may use at most 192 MiB of HBM per device.

```python
import jax
import jax.numpy as jnp
from jax import lax

EXPERTS = 128
D_MODEL = 2048
D_EXPERT = 768


def raised(result, rng, source, target, blocks, factor):
    def block_of(position):
        return (jnp.arange(result.shape[position]) // (result.shape[position] // blocks)).reshape((-1,) + (1,) * (result.ndim - 1 - position))

    near = jax.random.permutation(rng, blocks)[block_of(target)]
    other_side = (block_of(target) + blocks // 2) % blocks
    return jnp.where((block_of(source) == near) | (block_of(source) == other_side), factor * result, result)


def levels(rng, shape, split, smallest, largest):
    gain = 1.0
    for axis_at, blocks in split:
        draws = jax.random.uniform(jax.random.fold_in(jax.random.fold_in(rng, 6), axis_at), (blocks,), jnp.float32, smallest / len(split), largest / len(split))
        gain = gain * jnp.repeat(jnp.exp(draws), shape[axis_at] // blocks).reshape((-1,) + (1,) * (len(shape) - 1 - axis_at))
    return gain


def scatter_about(rng, shape, deviation, most, split=(), kind=jnp.bfloat16):
    entries = jax.random.normal(rng, shape, jnp.float32) * deviation
    if len(split) > 0:
        entries = levels(rng, shape, split, -0.22, 0.18) * entries
    return jnp.clip(entries, min=-most, max=most).astype(kind)


def heavy_noise(key, shape, scale, most, shards, heavy, kind=jnp.bfloat16):
    values = scale * jax.random.normal(key, shape, jnp.float32)
    if shards:
        values = values * levels(key, shape, shards, -0.22, 0.18)
    return jnp.clip(raised(values, jax.random.fold_in(key, 3), *heavy), -most, most).astype(kind)


def setup_inputs(seed: int = 0) -> dict:
    splits = jax.random.split(jax.random.key(seed), 7)
    train_gate = heavy_noise(splits[0], (EXPERTS, D_MODEL, D_EXPERT), D_MODEL ** -0.5, 0.1875, ((0, 4), (1, 8)), (1, 2, 8, 2.0), jnp.float32)
    other_gate = scatter_about(splits[1], (EXPERTS, D_MODEL, D_EXPERT), (D_MODEL * 4) ** -0.5, 0.0625, ((0, 4), (1, 8)))
    train_up = heavy_noise(splits[2], (EXPERTS, D_MODEL, D_EXPERT), D_MODEL ** -0.5, 0.1875, ((0, 4), (1, 8)), (1, 2, 8, 2.0), jnp.float32)
    other_up = scatter_about(splits[3], (EXPERTS, D_MODEL, D_EXPERT), (D_MODEL * 4) ** -0.5, 0.0625, ((0, 4), (1, 8)))
    router_weight = scatter_about(splits[4], (D_MODEL, EXPERTS), D_MODEL ** -0.5, 0.125, ((0, 8), (1, 4)), jnp.float32)
    router_gain = jnp.clip(1.0 + 0.15 * jax.random.normal(splits[5], (D_MODEL,), jnp.float32), 0.25, 1.75)
    return {"train_gate": train_gate, "other_gate": other_gate, "train_up": train_up, "other_up": other_up, "router_weight": router_weight, "router_gain": router_gain}


def reference(train_gate, other_gate, train_up, other_up, router_weight, router_gain):
    latest_gate = train_gate + other_gate.astype(jnp.float32)
    latest_up = train_up + other_up.astype(jnp.float32)
    scale_gate = jnp.sqrt(lax.optimization_barrier(jnp.sum(latest_gate * latest_gate, axis=1)))
    ready_gate = (latest_gate / jnp.expand_dims(scale_gate, 1)).astype(jnp.bfloat16)
    scale_up = jnp.sqrt(lax.optimization_barrier(jnp.sum(latest_up * latest_up, axis=1)))
    ready_up = (latest_up / jnp.expand_dims(scale_up, 1)).astype(jnp.bfloat16)
    serve_router = (router_weight * router_gain[:, None]).astype(jnp.bfloat16)
    return (ready_gate, ready_up, scale_gate, scale_up, serve_router)
```

```python
import functools

import jax
import jax.numpy as jnp
from jax import lax
from jax.experimental import pallas as pl
from jax.experimental.pallas import tpu as pltpu
from jax.sharding import PartitionSpec as P

VMEM_LIMIT = 48 * 1024 * 1024


def narrow_kernel(kinds, *refs):
    out_ref = refs[-1]
    for kind in range(kinds):
        train_ref, other_ref = refs[2 * kind], refs[2 * kind + 1]
        out_ref[0, 0, kind] = (
            train_ref[0, 0] + other_ref[0, 0].astype(jnp.float32)
        ).astype(jnp.bfloat16)


def narrow(arrays, firsts, count):
    kinds = len(firsts)
    zero, _, rows, cols = arrays[0].shape
    specs = [
        pl.BlockSpec((1, 1, rows, cols), lambda d, e, first=first: (d, first + e, 0, 0))
        for first in firsts
        for _ in range(2)
    ]
    size = zero * count * kinds * rows * cols
    return pl.pallas_call(
        functools.partial(narrow_kernel, kinds),
        grid=(zero, count),
        in_specs=specs,
        out_specs=pl.BlockSpec((1, 1, kinds, rows, cols), lambda d, e: (d, e, 0, 0, 0)),
        out_shape=jax.ShapeDtypeStruct((zero, count, kinds, rows, cols), jnp.bfloat16),
        compiler_params=pltpu.CompilerParams(vmem_limit_bytes=VMEM_LIMIT),
        cost_estimate=pl.CostEstimate(flops=size, bytes_accessed=8 * size, transcendentals=0),
    )(*arrays)


def normalise_kernel(parts, rows, kinds, x_ref, *refs):
    outs = refs[-2 * kinds :]
    for kind in range(kinds):
        ready_ref, scale_ref = outs[kind], outs[kinds + kind]
        total = jnp.zeros((1, x_ref.shape[-1]), jnp.float32)
        for part in range(parts):
            x = x_ref[part, 0, kind].astype(jnp.float32)
            total = total + jnp.sum(x * x, axis=0, keepdims=True)
        scale = jnp.sqrt(total)
        scale_ref[0] = scale
        inverse = 1.0 / scale
        for part in range(parts):
            x = x_ref[part, 0, kind].astype(jnp.float32)
            ready_ref[0, pl.ds(part * rows, rows), :] = (x * inverse).astype(jnp.bfloat16)


def normalise(arrived, ready, firsts, local):
    parts, count, kinds, rows, cols = arrived.shape
    tile = cols // 3 if cols % 384 == 0 else cols
    spec = pl.BlockSpec((parts, 1, kinds, rows, tile), lambda e, j: (0, e, 0, 0, j))
    out_ready = [
        pl.BlockSpec((1, parts * rows, tile), lambda e, j, first=first: (first + e, 0, j))
        for first in firsts
    ]
    out_scale = pl.BlockSpec((1, 1, tile), lambda e, j: (e, 0, j))
    full = jax.ShapeDtypeStruct((local, parts * rows, cols), jnp.bfloat16)
    scales = jax.ShapeDtypeStruct((count, 1, cols), jnp.float32)
    held = [(kind, array) for kind, array in enumerate(ready) if array is not None]
    size = parts * count * kinds * rows * cols
    out = pl.pallas_call(
        functools.partial(normalise_kernel, parts, rows, kinds),
        grid=(count, cols // tile),
        in_specs=[spec] + [pl.BlockSpec(memory_space=pl.ANY)] * len(held),
        out_specs=out_ready + [out_scale] * kinds,
        out_shape=[full] * kinds + [scales] * kinds,
        input_output_aliases={1 + i: kind for i, (kind, _) in enumerate(held)},
        compiler_params=pltpu.CompilerParams(vmem_limit_bytes=VMEM_LIMIT),
        cost_estimate=pl.CostEstimate(flops=4 * size, bytes_accessed=4 * size, transcendentals=0),
    )(arrived, *(array for _, array in held))
    return out[:kinds], out[kinds:]


def rows_from_all(part, zero):
    me = lax.axis_index("zero")
    pieces = [part] + [
        lax.ppermute(part, "zero", [(i, (i + k) % zero) for i in range(zero)])
        for k in range(1, zero)
    ]
    return [(lax.rem(me + zero - k, zero), piece) for k, piece in enumerate(pieces)]


def router_of(placed, pieces, zero):
    columns, rows = pieces[0].shape
    row = jnp.zeros((zero, columns, rows), jnp.bfloat16)
    for (source, _), piece in zip(placed, pieces):
        row = lax.dynamic_update_slice(row, piece[None], (source, 0, 0))
    row = row.transpose(1, 0, 2).reshape(columns, zero * rows)
    return lax.all_gather(row, "bank", axis=0, tiled=True).T


def body(zero, train_gate, other_gate, train_up, other_up, router_weight, router_gain):
    experts, rows, cols = train_gate.shape
    local = experts // zero
    gate = [a.reshape(zero, local, rows, cols) for a in (train_gate, other_gate)]
    up = [a.reshape(zero, local, rows, cols) for a in (train_up, other_up)]

    plan = [((0,), (0,), 1), ((0, 1), (1, 0), local - 1), ((1,), (local - 1,), 1)]
    plan = [step for step in plan if step[2] > 0]

    part = (router_weight * router_gain[:, None]).astype(jnp.bfloat16).T

    ready, scales = [None, None], [[], []]
    for at, (kinds, firsts, count) in enumerate(plan):
        sent = narrow([a for kind in kinds for a in (gate, up)[kind]], firsts, count)
        if at == 1:
            sent, part = lax.optimization_barrier((sent, part))
            placed = rows_from_all(part, zero)
            sent, pieces = lax.optimization_barrier((sent, [piece for _, piece in placed]))
        if at == 2:
            sent, pieces = lax.optimization_barrier((sent, pieces))
            serve_router = router_of(placed, pieces, zero)
            sent, serve_router = lax.optimization_barrier((sent, serve_router))
        arrived = lax.all_to_all(sent, "zero", split_axis=0, concat_axis=0, tiled=True)
        new_ready, new_scales = normalise(arrived, [ready[kind] for kind in kinds], firsts, local)
        for kind, array, scale in zip(kinds, new_ready, new_scales):
            ready[kind] = array
            scales[kind].append(scale)
    if len(plan) < 3:
        serve_router = router_of(placed, pieces, zero)
    return (
        ready[0],
        ready[1],
        jnp.concatenate(scales[0]).reshape(local, cols),
        jnp.concatenate(scales[1]).reshape(local, cols),
        serve_router,
    )


def solution(mesh):
    placed = (
        P("bank", "zero", None),
        P("bank", "zero", None),
        P("bank", "zero", None),
        P("bank", "zero", None),
        P("zero", "bank"),
        P("zero"),
    )
    return jax.shard_map(
        functools.partial(body, mesh.shape["zero"]),
        mesh=mesh,
        in_specs=placed,
        out_specs=(
            P(("bank", "zero"), None, None),
            P(("bank", "zero"), None, None),
            P(("bank", "zero"), None),
            P(("bank", "zero"), None),
            P(),
        ),
        check_vma=False,
    )
```
